32 devices in a mesh: rep: 2 (over y), fsdp: 16 (over z, x, core).
Axes of the slice: x: 2, y: 2, z: 4, core: 2. Of those that a mesh axis runs over, the one named last changes fastest.
Arguments:
- tokens: bfloat16 [16384, 4096], P(('rep', 'fsdp')), may hold values from -6 to 6
- value_cot: bfloat16 [16384, 1024], P(('rep', 'fsdp')), may hold values from -6 to 6
- value_weight: bfloat16 [2, 4096, 1024], P('rep', 'fsdp'), may hold values from -0.09375 to 0.09375
- global_params: float32 [2097152], P('fsdp'), may hold values from -6 to 6
- local_params: float32 [2, 2097152], P('rep', 'fsdp'), may hold values from -6 to 6
- momentum: float32 [2097152], P('fsdp'), may hold values from -3 to 3
Outputs:
- token_grad: bfloat16 [16384, 4096], P(('rep', 'fsdp'))
- value_grad: float32 [2, 4096, 1024], P('rep', 'fsdp')
- new_global: float32 [2097152], P('fsdp')
- new_moment: float32 [2097152], P('fsdp')
The draws below stay inside these ranges and needn't reach their ends.
All inputs are finite; a program needn't handle non-finite values.
Results may differ from the reference program's by a relative error of at most 0.001.
Values may be sent and summed in bfloat16 or wider, within the bound.
A program may use at most 128 MiB of HBM per device.

```python
import jax
import jax.numpy as jnp
from jax import lax

D = 4096
KVW = 1024
REPS = 2
GROUP_TOK = 8192
TOKENS = 16384
FRAG = 2097152
N_REP = 2


def spiked(drawn, rng, source, target, shards_of, factor):
    def block_of(dim):
        return (jnp.arange(drawn.shape[dim]) // (drawn.shape[dim] // shards_of)).reshape((-1,) + (1,) * (drawn.ndim - 1 - dim))

    first = jax.random.permutation(rng, shards_of)[block_of(target)]
    far = (block_of(target) + shards_of // 2) % shards_of
    return jnp.where((block_of(source) == first) | (block_of(source) == far), factor * drawn, drawn)


def block_levels(stream_key, extent, shards, smallest, top_value):
    def one(dim, shards_of):
        draws = jax.random.uniform(jax.random.fold_in(jax.random.fold_in(stream_key, 6), dim), (shards_of,), jnp.float32, smallest / len(shards), top_value / len(shards))
        return jnp.repeat(jnp.exp(draws), extent[dim] // shards_of).reshape((-1,) + (1,) * (len(extent) - dim - 1))

    level = one(*shards[0])
    for cut in shards[1:]:
        level = level * one(*cut)
    return level


def noise(key, dims, spread, reach, pieces=(), held_as=jnp.bfloat16):
    drawn = spread * jax.random.normal(key, dims, jnp.float32)
    if pieces:
        drawn = drawn * block_levels(key, dims, pieces, -0.22, 0.18)
    return jnp.clip(drawn, -reach, reach).astype(held_as)


def heavy_noise(stream_key, dims, scale, reach, pieces, heavy, dtype=jnp.bfloat16):
    array = scale * jax.random.normal(stream_key, dims, jnp.float32)
    if pieces:
        array = array * block_levels(stream_key, dims, pieces, -0.22, 0.18)
    return jnp.clip(spiked(array, jax.random.fold_in(stream_key, 3), *heavy), -reach, reach).astype(dtype)


def setup_inputs(seed: int = 0) -> dict:
    keys = jax.random.split(jax.random.key(seed), 7)
    return {
        "tokens": heavy_noise(keys[0], (TOKENS, D), 1.0, 6.0, ((0, 32),), (0, 1, 32, 2.75)),
        "value_cot": noise(keys[1], (TOKENS, KVW), 1.0, 6.0, ((0, 32),)),
        "value_weight": noise(keys[2], (REPS, D, KVW), D ** -0.5, 0.09375, ((0, 2), (1, 16))),
        "global_params": noise(keys[3], (FRAG,), 1.0, 6.0, ((0, 16),), jnp.float32),
        "local_params": noise(keys[4], (REPS, FRAG), 1.0, 6.0, ((0, 2), (1, 16)), jnp.float32),
        "momentum": noise(keys[5], (FRAG,), 0.5, 3.0, ((0, 16),), jnp.float32),
    }


def reference(tokens, value_cot, value_weight, global_params, local_params, momentum):
    token_parts = []
    grad_parts = []
    for replica in range(N_REP):
        inputs = tokens[replica * GROUP_TOK:(replica + 1) * GROUP_TOK]
        cotan = value_cot[replica * GROUP_TOK:(replica + 1) * GROUP_TOK]
        token_parts.append(jnp.dot(cotan, value_weight[replica].T, preferred_element_type=jnp.float32).astype(jnp.bfloat16))
        summed = jnp.dot(inputs.T, cotan, preferred_element_type=jnp.float32)
        grad_parts.append(summed * (1.0 / jnp.sqrt(jnp.float32(GROUP_TOK))))
    token_grad = jnp.concatenate(token_parts, axis=0)
    value_grad = jnp.stack(grad_parts, axis=0)
    pseudo = global_params - lax.optimization_barrier(jnp.sum(local_params, axis=0)) / N_REP
    new_moment = 0.9 * momentum + pseudo
    new_global = global_params - 0.7 * (pseudo + 0.9 * new_moment)
    return (token_grad, value_grad, new_global, new_moment)
```

```python
import functools

import jax
import jax.numpy as jnp
from jax import lax
from jax.experimental import pallas as pl
from jax.experimental.pallas import tpu as pltpu
from jax.sharding import PartitionSpec as P

CORES = 2
COLS = 2
SCALE = 2.0 ** 8


def grad_term(tokens, columns):
    return lax.dot_general(
        tokens, columns, (((0,), (0,)), ((), ())), preferred_element_type=jnp.float32
    )


def pack(v):
    v = v * SCALE
    v = v * jnp.abs(v)
    return (v * jnp.abs(v)).astype(jnp.bfloat16)


def unpack(p):
    p = p.astype(jnp.float32)
    r = jnp.sqrt(jnp.sqrt(jnp.abs(p))) * (1.0 / SCALE)
    return jnp.where(p < 0, -r, r)


def kernel(groups, factor, x_ref, c_ref, w_ref, tg_ref, vg_ref,
           wbuf, xr, cr, acc_a, acc_b, sax, rax, saz, raz, sbz, rbz, sbx, rbx,
           rw, szr, szl, sx, sc, xs, xrs, cs, own_sem, axs, axr, azs, azr, bzs, bzr, bxs):
    nz = groups // (CORES * COLS)
    f = lax.axis_index("fsdp")
    core, x, z = lax.rem(f, CORES), lax.rem(f // CORES, COLS), f // (CORES * COLS)
    depth = w_ref.shape[0]
    half = depth // 2
    wide = c_ref.shape[1] // 2

    def ident(zz, xx, cc):
        return (zz * COLS + xx) * CORES + cc

    ox, oc = 1 - x, 1 - core
    xdev, cdev = ident(z, ox, core), ident(z, x, oc)
    rdev, ldev = ident(z + 1, x, core), ident(z - 1, x, core)
    has_r, has_l = z < nz - 1, z > 0

    def both(fn):
        pl.when(has_r)(lambda: fn(rdev))
        pl.when(has_l)(lambda: fn(ldev))

    barrier = pltpu.get_barrier_semaphore()

    def greet(dev):
        pl.semaphore_signal(barrier, inc=1, device_id={"fsdp": dev}, device_id_type=pl.DeviceIdType.MESH)

    own = pltpu.make_async_copy(w_ref, wbuf.at[f], own_sem)
    own.start()
    greet(xdev)
    greet(cdev)
    both(greet)
    pl.semaphore_wait(barrier, 2 + jnp.where(has_r, 1, 0) + jnp.where(has_l, 1, 0))

    def remote(src, dst, ssem, rsem, dev):
        return pltpu.make_async_remote_copy(
            src_ref=src, dst_ref=dst, send_sem=ssem, recv_sem=rsem,
            device_id={"fsdp": dev}, device_id_type=pl.DeviceIdType.MESH)

    cot = remote(c_ref, cr, cs.at[0], cs.at[1], cdev)
    cot.start()

    def xcopy(q):
        d = q * CORES + oc
        return remote(x_ref.at[:, pl.ds(pl.multiple_of(d * depth, depth), depth)], xr.at[q], xs.at[q], xrs.at[q], cdev)

    nq = nz * COLS

    @pl.loop(0, nq)
    def _(q):
        xcopy(q).start()

    own.wait()

    def piece(h, blk, ssem, dev):
        part = wbuf.at[blk, pl.ds(h * half, half)]
        return remote(part, part, ssem.at[h, blk], rw.at[h, blk], dev)

    def right(h, blk):
        return piece(h, blk, szr, rdev)

    def left(h, blk):
        return piece(h, blk, szl, ldev)

    def across(h, blk):
        return piece(h, blk, sx, xdev)

    def core_way(h, blk):
        return piece(h, blk, sc, cdev)

    def send_z(h, blk):
        pl.when(has_r)(lambda: right(h, blk).start())
        pl.when(has_l)(lambda: left(h, blk).start())

    across(1, f).start()
    send_z(0, f)
    send_z(1, f)
    across(0, f).start()
    core_way(0, f).start()
    core_way(1, f).start()

    cot.wait_recv()

    @pl.loop(0, nq)
    def _(q):
        xcopy(q).wait_recv()

    def grad(zz, xx):
        q = zz * COLS + xx
        d = ident(zz, xx, core)
        cols = pl.ds(pl.multiple_of(d * depth, depth), depth)
        return grad_term(x_ref[:, cols], c_ref[...]) + grad_term(xr[q], cr[...])

    def ax(zz):
        return remote(sax.at[zz], rax.at[zz], axs.at[zz], axr.at[zz], xdev)

    @pl.loop(0, nz)
    def _(zz):
        g = grad(zz, ox)
        sax[zz] = pack(g[:, :wide])
        ax(zz).start()
        acc_b[zz, ox] = g[:, wide:]

    other = ident(z, ox, core)
    across(1, other).wait_recv()
    send_z(1, other)
    core_way(1, other).start()

    @pl.loop(0, nz)
    def _(zz):
        g = grad(zz, x)
        acc_a[zz] = g[:, :wide]
        acc_b[zz, x] = g[:, wide:]

    def hop(k):
        for h in range(2):
            for ok, zo, fwd, nxt in ((z - k >= 0, z - k, right, has_r), (z + k < nz, z + k, left, has_l)):
                @pl.when(ok)
                def _():
                    for xx in ((x,) if h == 0 else (x, ox)):
                        blk = ident(zo, xx, core)
                        fwd(h, blk).wait_recv()
                        pl.when(nxt)(lambda: fwd(h, blk).start())
                        if h == 0:
                            across(h, blk).start()
                        core_way(h, blk).start()

    def line(acc, sbuf, rbuf, ssem, rsem):
        def copy(way, zz):
            return remote(sbuf.at[zz], rbuf.at[way, zz], ssem.at[zz], rsem.at[way, zz], rdev if way == 0 else ldev)

        def step(j):
            for way, zz, more, mine, came in (
                (0, nz - 1 - j, nz - 1 - j > z, nz - 1 - j == z, has_l),
                (1, j, j < z, j == z, has_r),
            ):
                @pl.when(jnp.logical_and(jnp.logical_or(more, mine), came))
                def _():
                    copy(way, zz).wait_recv()
                    acc[zz] += unpack(rbuf[way, zz])

                @pl.when(more)
                def _():
                    sbuf[zz] = pack(acc[zz])
                    copy(way, zz).start()

        def drain():
            for zz in range(nz):
                pl.when(zz > z)(lambda: copy(0, zz).wait_send())
                pl.when(zz < z)(lambda: copy(1, zz).wait_send())

        return step, drain

    step_a, drain_a = line(acc_a, saz, raz, azs, azr)
    step_b, drain_b = line(acc_b, sbz, rbz, bzs, bzr)

    hop(1)
    step_b(0)
    hop(2) if nz > 2 else None

    @pl.loop(0, nz)
    def _(zz):
        ax(zz).wait_recv()
        acc_a[zz] += unpack(rax[zz])

    for j in range(1, nz):
        step_a(j - 1)
        if j + 2 < nz:
            hop(j + 2)
        step_b(j)
    bx = remote(sbx, rbx, bxs.at[0], bxs.at[1], xdev)
    sbx[...] = pack(acc_b[z, ox])
    bx.start()
    step_a(nz - 1)

    for zo in range(nz):
        blk = ident(zo, ox, core)
        across(0, blk).wait_recv()
        core_way(0, blk).start()

    def project(d):
        tg_ref[:, pl.ds(pl.multiple_of(d * depth, depth), depth)] = lax.dot_general(
            c_ref[...], wbuf[d], (((1,), (1,)), ((), ())), preferred_element_type=jnp.float32
        ).astype(jnp.bfloat16)

    @pl.loop(0, nq)
    def _(q):
        project(q * CORES + core)

    vg_ref[:, :wide] = acc_a[z] * factor
    bx.wait_recv()
    vg_ref[:, wide:] = (acc_b[z, x] + unpack(rbx[...])) * factor

    @pl.loop(0, nq)
    def _(q):
        d = q * CORES + oc
        core_way(0, d).wait_recv()
        core_way(1, d).wait_recv()
        project(d)

    cot.wait_send()
    bx.wait_send()
    drain_a()
    drain_b()

    @pl.loop(0, nq)
    def _(q):
        xcopy(q).wait_send()
        d = q * CORES + core
        core_way(0, d).wait_send()
        core_way(1, d).wait_send()

    across(1, f).wait_send()

    @pl.loop(0, nz)
    def _(zz):
        ax(zz).wait_send()
        across(0, ident(zz, x, core)).wait_send()
        go_r = jnp.logical_and(zz <= z, has_r)
        go_l = jnp.logical_and(zz >= z, has_l)
        for h, xx in ((0, x), (1, x), (1, ox)):
            pl.when(go_r)(lambda: right(h, ident(zz, xx, core)).wait_send())
            pl.when(go_l)(lambda: left(h, ident(zz, xx, core)).wait_send())


def fused(tokens, value_cot, weight, groups, factor):
    nz = groups // (CORES * COLS)
    rows, wide = tokens.shape[0], value_cot.shape[1]
    depth = weight.shape[0]
    w2 = wide // 2
    bf, f32 = jnp.bfloat16, jnp.float32
    dma = pltpu.SemaphoreType.DMA
    vmem = pl.BlockSpec(memory_space=pltpu.VMEM)
    return pl.pallas_call(
        functools.partial(kernel, groups, factor),
        out_shape=(
            jax.ShapeDtypeStruct((rows, tokens.shape[1]), bf),
            jax.ShapeDtypeStruct((depth, wide), f32),
        ),
        in_specs=[vmem] * 3,
        out_specs=(vmem, vmem),
        scratch_shapes=[
            pltpu.VMEM((groups, depth, wide), bf),
            pltpu.VMEM((nz * COLS, rows, depth), bf),
            pltpu.VMEM((rows, wide), bf),
            pltpu.VMEM((nz, depth, w2), f32),
            pltpu.VMEM((nz, COLS, depth, w2), f32),
            pltpu.VMEM((nz, depth, w2), bf),
            pltpu.VMEM((nz, depth, w2), bf),
            pltpu.VMEM((nz, depth, w2), bf),
            pltpu.VMEM((2, nz, depth, w2), bf),
            pltpu.VMEM((nz, COLS, depth, w2), bf),
            pltpu.VMEM((2, nz, COLS, depth, w2), bf),
            pltpu.VMEM((depth, w2), bf),
            pltpu.VMEM((depth, w2), bf),
            dma((2, groups)), dma((2, groups)), dma((2, groups)), dma((2, groups)), dma((2, groups)),
            dma((nz * COLS,)), dma((nz * COLS,)), dma((2,)), dma,
            dma((nz,)), dma((nz,)), dma((nz,)), dma((2, nz)), dma((nz,)), dma((2, nz)), dma((2,)),
        ],
        compiler_params=pltpu.CompilerParams(
            collective_id=0, has_side_effects=True, vmem_limit_bytes=56 * 1024 * 1024
        ),
        cost_estimate=pl.CostEstimate(flops=80_000_000_000, bytes_accessed=20_000_000, transcendentals=0),
    )(tokens, value_cot, weight)


def shards(tokens, value_cot, value_weight, global_params, local_params, momentum):
    weight = value_weight[0]
    groups = lax.axis_size("fsdp")
    reps = lax.axis_size("rep")
    local = local_params[0]
    factor = 1.0 / float(tokens.shape[0] * groups) ** 0.5
    if reps == 2:
        totals = local + lax.ppermute(local, "rep", [(0, 1), (1, 0)])
    else:
        totals = lax.psum(local, "rep")
    depth = weight.shape[0]
    if depth % 128 == 0 and groups % (CORES * COLS) == 0 and groups > CORES * COLS:
        token_grad, value_grad = fused(tokens, value_cot, weight, groups, factor)
    else:
        token_grad = lax.dot_general(
            value_cot,
            lax.all_gather(weight, "fsdp", axis=0, tiled=True),
            (((1,), (1,)), ((), ())),
            preferred_element_type=jnp.float32,
        ).astype(jnp.bfloat16)
        value_grad = factor * lax.psum_scatter(
            grad_term(tokens, value_cot), "fsdp", scatter_dimension=0, tiled=True
        )
    pseudo = global_params - totals / reps
    new_moment = 0.9 * momentum + pseudo
    new_global = global_params - 0.7 * (pseudo + 0.9 * new_moment)
    return (token_grad, value_grad[None], new_global, new_moment)


def solution(mesh):
    in_specs = (
        P(("rep", "fsdp"), None),
        P(("rep", "fsdp"), None),
        P("rep", "fsdp", None),
        P("fsdp"),
        P("rep", "fsdp"),
        P("fsdp"),
    )
    out_specs = (P(("rep", "fsdp"), None), P("rep", "fsdp", None), P("fsdp"), P("fsdp"))
    return jax.shard_map(shards, mesh=mesh, in_specs=in_specs, out_specs=out_specs, check_vma=False)
```

```python
import functools

import jax
import jax.numpy as jnp
from jax import lax
from jax.experimental import pallas as pl
from jax.experimental.pallas import tpu as pltpu
from jax.sharding import PartitionSpec as P

CORES = 2
COLS = 2
SCALE = 2.0 ** 8


def grad_term(tokens, columns):
    return lax.dot_general(
        tokens, columns, (((0,), (0,)), ((), ())), preferred_element_type=jnp.float32
    )


def pack(v):
    v = v * SCALE
    v = v * jnp.abs(v)
    return (v * jnp.abs(v)).astype(jnp.bfloat16)


def unpack(p):
    p = p.astype(jnp.float32)
    r = jnp.sqrt(jnp.sqrt(jnp.abs(p))) * (1.0 / SCALE)
    return jnp.where(p < 0, -r, r)


def kernel(groups, factor, x_ref, c_ref, w_ref, tg_ref, vg_ref,
           wbuf, xr, cr, acc_a, acc_b, sax, rax, saz, raz, sbz, rbz, sbx, rbx,
           rw, szr, szl, sx, sc, xs, xrs, cs, own_sem, axs, axr, azs, azr, bzs, bzr, bxs):
    nz = groups // (CORES * COLS)
    f = lax.axis_index("fsdp")
    core, x, z = lax.rem(f, CORES), lax.rem(f // CORES, COLS), f // (CORES * COLS)
    depth = w_ref.shape[0]
    half = depth // 2
    wide = c_ref.shape[1] // 2

    def ident(zz, xx, cc):
        return (zz * COLS + xx) * CORES + cc

    ox, oc = 1 - x, 1 - core
    xdev, cdev = ident(z, ox, core), ident(z, x, oc)
    rdev, ldev = ident(z + 1, x, core), ident(z - 1, x, core)
    has_r, has_l = z < nz - 1, z > 0

    def both(fn):
        pl.when(has_r)(lambda: fn(rdev))
        pl.when(has_l)(lambda: fn(ldev))

    barrier = pltpu.get_barrier_semaphore()

    def greet(dev):
        pl.semaphore_signal(barrier, inc=1, device_id={"fsdp": dev}, device_id_type=pl.DeviceIdType.MESH)

    own = pltpu.make_async_copy(w_ref, wbuf.at[f], own_sem)
    own.start()
    greet(xdev)
    greet(cdev)
    both(greet)
    pl.semaphore_wait(barrier, 2 + jnp.where(has_r, 1, 0) + jnp.where(has_l, 1, 0))

    def remote(src, dst, ssem, rsem, dev):
        return pltpu.make_async_remote_copy(
            src_ref=src, dst_ref=dst, send_sem=ssem, recv_sem=rsem,
            device_id={"fsdp": dev}, device_id_type=pl.DeviceIdType.MESH)

    cot = remote(c_ref, cr, cs.at[0], cs.at[1], cdev)
    cot.start()

    def xcopy(q):
        d = q * CORES + oc
        return remote(x_ref.at[:, pl.ds(pl.multiple_of(d * depth, depth), depth)], xr.at[q], xs.at[q], xrs.at[q], cdev)

    nq = nz * COLS

    @pl.loop(0, nq)
    def _(q):
        xcopy(q).start()

    own.wait()

    def piece(h, blk, ssem, dev):
        part = wbuf.at[blk, pl.ds(h * half, half)]
        return remote(part, part, ssem.at[h, blk], rw.at[h, blk], dev)

    def right(h, blk):
        return piece(h, blk, szr, rdev)

    def left(h, blk):
        return piece(h, blk, szl, ldev)

    def across(h, blk):
        return piece(h, blk, sx, xdev)

    def core_way(h, blk):
        return piece(h, blk, sc, cdev)

    def send_z(h, blk):
        pl.when(has_r)(lambda: right(h, blk).start())
        pl.when(has_l)(lambda: left(h, blk).start())

    across(1, f).start()
    send_z(0, f)
    send_z(1, f)
    core_way(0, f).start()
    core_way(1, f).start()

    cot.wait_recv()

    @pl.loop(0, nq)
    def _(q):
        xcopy(q).wait_recv()

    def grad(zz, xx):
        q = zz * COLS + xx
        d = ident(zz, xx, core)
        cols = pl.ds(pl.multiple_of(d * depth, depth), depth)
        return grad_term(x_ref[:, cols], c_ref[...]) + grad_term(xr[q], cr[...])

    def ax(zz):
        return remote(sax.at[zz], rax.at[zz], axs.at[zz], axr.at[zz], xdev)

    @pl.loop(0, nz)
    def _(zz):
        g = grad(zz, ox)
        sax[zz] = pack(g[:, :wide])
        ax(zz).start()
        acc_b[zz, ox] = g[:, wide:]

    across(0, f).start()

    other = ident(z, ox, core)
    across(1, other).wait_recv()
    send_z(1, other)
    core_way(1, other).start()

    @pl.loop(0, nz)
    def _(zz):
        g = grad(zz, x)
        acc_a[zz] = g[:, :wide]
        acc_b[zz, x] = g[:, wide:]

    def hop(k):
        for h in range(2):
            for ok, zo, fwd, nxt in ((z - k >= 0, z - k, right, has_r), (z + k < nz, z + k, left, has_l)):
                @pl.when(ok)
                def _():
                    for xx in ((x,) if h == 0 else (x, ox)):
                        blk = ident(zo, xx, core)
                        fwd(h, blk).wait_recv()
                        pl.when(nxt)(lambda: fwd(h, blk).start())
                        if h == 0:
                            across(h, blk).start()
                        core_way(h, blk).start()

    def line(acc, sbuf, rbuf, ssem, rsem):
        def copy(way, zz):
            return remote(sbuf.at[zz], rbuf.at[way, zz], ssem.at[zz], rsem.at[way, zz], rdev if way == 0 else ldev)

        def step(s):
            late = nz - 1 - s
            for way, zz, ok, came in ((0, z + late, z <= s, has_l), (1, z - late, nz - 1 - z <= s, has_r)):
                @pl.when(jnp.logical_and(ok, came))
                def _():
                    copy(way, zz).wait_recv()
                    acc[zz] += unpack(rbuf[way, zz])

                if late:
                    @pl.when(ok)
                    def _():
                        sbuf[zz] = pack(acc[zz])
                        copy(way, zz).start()

        def drain():
            for zz in range(nz):
                pl.when(zz > z)(lambda: copy(0, zz).wait_send())
                pl.when(zz < z)(lambda: copy(1, zz).wait_send())

        return step, drain

    step_a, drain_a = line(acc_a, saz, raz, azs, azr)
    step_b, drain_b = line(acc_b, sbz, rbz, bzs, bzr)

    step_b(0)
    for s in range(1, nz):
        hop(s)
        step_b(s)
        if s == 1:
            @pl.loop(0, nz)
            def _(zz):
                ax(zz).wait_recv()
                acc_a[zz] += unpack(rax[zz])
        if s == nz - 1:
            bx = remote(sbx, rbx, bxs.at[0], bxs.at[1], xdev)
            sbx[...] = pack(acc_b[z, ox])
            bx.start()
        step_a(s - 1)

    for zo in range(nz):
        blk = ident(zo, ox, core)
        across(0, blk).wait_recv()
        core_way(0, blk).start()

    def project(d):
        tg_ref[:, pl.ds(pl.multiple_of(d * depth, depth), depth)] = lax.dot_general(
            c_ref[...], wbuf[d], (((1,), (1,)), ((), ())), preferred_element_type=jnp.float32
        ).astype(jnp.bfloat16)

    @pl.loop(0, nq)
    def _(q):
        project(q * CORES + core)

    step_a(nz - 1)
    vg_ref[:, :wide] = acc_a[z] * factor
    bx.wait_recv()
    vg_ref[:, wide:] = (acc_b[z, x] + unpack(rbx[...])) * factor

    @pl.loop(0, nq)
    def _(q):
        d = q * CORES + oc
        core_way(0, d).wait_recv()
        core_way(1, d).wait_recv()
        project(d)

    cot.wait_send()
    bx.wait_send()
    drain_a()
    drain_b()

    @pl.loop(0, nq)
    def _(q):
        xcopy(q).wait_send()
        d = q * CORES + core
        core_way(0, d).wait_send()
        core_way(1, d).wait_send()

    across(1, f).wait_send()

    @pl.loop(0, nz)
    def _(zz):
        ax(zz).wait_send()
        across(0, ident(zz, x, core)).wait_send()
        go_r = jnp.logical_and(zz <= z, has_r)
        go_l = jnp.logical_and(zz >= z, has_l)
        for h, xx in ((0, x), (1, x), (1, ox)):
            pl.when(go_r)(lambda: right(h, ident(zz, xx, core)).wait_send())
            pl.when(go_l)(lambda: left(h, ident(zz, xx, core)).wait_send())


def fused(tokens, value_cot, weight, groups, factor):
    nz = groups // (CORES * COLS)
    rows, wide = tokens.shape[0], value_cot.shape[1]
    depth = weight.shape[0]
    w2 = wide // 2
    bf, f32 = jnp.bfloat16, jnp.float32
    dma = pltpu.SemaphoreType.DMA
    vmem = pl.BlockSpec(memory_space=pltpu.VMEM)
    return pl.pallas_call(
        functools.partial(kernel, groups, factor),
        out_shape=(
            jax.ShapeDtypeStruct((rows, tokens.shape[1]), bf),
            jax.ShapeDtypeStruct((depth, wide), f32),
        ),
        in_specs=[vmem] * 3,
        out_specs=(vmem, vmem),
        scratch_shapes=[
            pltpu.VMEM((groups, depth, wide), bf),
            pltpu.VMEM((nz * COLS, rows, depth), bf),
            pltpu.VMEM((rows, wide), bf),
            pltpu.VMEM((nz, depth, w2), f32),
            pltpu.VMEM((nz, COLS, depth, w2), f32),
            pltpu.VMEM((nz, depth, w2), bf),
            pltpu.VMEM((nz, depth, w2), bf),
            pltpu.VMEM((nz, depth, w2), bf),
            pltpu.VMEM((2, nz, depth, w2), bf),
            pltpu.VMEM((nz, COLS, depth, w2), bf),
            pltpu.VMEM((2, nz, COLS, depth, w2), bf),
            pltpu.VMEM((depth, w2), bf),
            pltpu.VMEM((depth, w2), bf),
            dma((2, groups)), dma((2, groups)), dma((2, groups)), dma((2, groups)), dma((2, groups)),
            dma((nz * COLS,)), dma((nz * COLS,)), dma((2,)), dma,
            dma((nz,)), dma((nz,)), dma((nz,)), dma((2, nz)), dma((nz,)), dma((2, nz)), dma((2,)),
        ],
        compiler_params=pltpu.CompilerParams(
            collective_id=0, has_side_effects=True, vmem_limit_bytes=56 * 1024 * 1024
        ),
        cost_estimate=pl.CostEstimate(flops=80_000_000_000, bytes_accessed=20_000_000, transcendentals=0),
    )(tokens, value_cot, weight)


def shards(tokens, value_cot, value_weight, global_params, local_params, momentum):
    weight = value_weight[0]
    groups = lax.axis_size("fsdp")
    reps = lax.axis_size("rep")
    local = local_params[0]
    factor = 1.0 / float(tokens.shape[0] * groups) ** 0.5
    if reps == 2:
        totals = local + lax.ppermute(local, "rep", [(0, 1), (1, 0)])
    else:
        totals = lax.psum(local, "rep")
    depth = weight.shape[0]
    if depth % 128 == 0 and groups % (CORES * COLS) == 0 and groups > CORES * COLS:
        token_grad, value_grad = fused(tokens, value_cot, weight, groups, factor)
    else:
        token_grad = lax.dot_general(
            value_cot,
            lax.all_gather(weight, "fsdp", axis=0, tiled=True),
            (((1,), (1,)), ((), ())),
            preferred_element_type=jnp.float32,
        ).astype(jnp.bfloat16)
        value_grad = factor * lax.psum_scatter(
            grad_term(tokens, value_cot), "fsdp", scatter_dimension=0, tiled=True
        )
    pseudo = global_params - totals / reps
    new_moment = 0.9 * momentum + pseudo
    new_global = global_params - 0.7 * (pseudo + 0.9 * new_moment)
    return (token_grad, value_grad[None], new_global, new_moment)


def solution(mesh):
    in_specs = (
        P(("rep", "fsdp"), None),
        P(("rep", "fsdp"), None),
        P("rep", "fsdp", None),
        P("fsdp"),
        P("rep", "fsdp"),
        P("fsdp"),
    )
    out_specs = (P(("rep", "fsdp"), None), P("rep", "fsdp", None), P("fsdp"), P("fsdp"))
    return jax.shard_map(shards, mesh=mesh, in_specs=in_specs, out_specs=out_specs, check_vma=False)
```
